32 devices in a mesh: tm: 4 (over z), env: 8 (over y, x, core).
Axes of the slice: x: 2, y: 2, z: 4, core: 2. Of those that a mesh axis runs over, the one named last changes fastest.
Arguments:
- rewards: float32 [1024, 1024], P('tm', 'env'), may hold values from -6 to 6
- dones: int32 [1024, 1024], P('tm', 'env'), may hold values 0 or 1
- horizon: float32 [1024], P('env'), may hold values from 20 to 2048
- bootstrap: float32 [1024], P('env'), may hold values from -96 to 96
- prior_mean: float32 [1], replicated, may hold values from -240 to 240
- prior_var: float32 [1], replicated, may hold values from 100 to 3000
Outputs:
- scaled_rewards: float32 [1024, 1024], P('tm', 'env')
- scaled_returns: float32 [1024, 1024], P('tm', 'env')
- running_stats: float32 [2], replicated
The draws below stay inside these ranges and needn't reach their ends.
All inputs are finite; a program needn't handle non-finite values. No bound on the sum of `dones` on one device may be relied on, other than what follows from the above.
Results may differ from the reference program's by a relative error of at most 0.0003.
Values sent between devices are 32-bit elements; how exact they have to be, the bound alone decides.
A program may use at most 64 MiB of HBM per device.

```python
import math
import jax
import jax.numpy as jnp
from jax import lax

TIME = 1024
ENVS = 1024
PRIOR = 1048576


def place_ends(result, key, least, largest):
    place = [jax.random.randint(jax.random.fold_in(key, axis), (), 0, length) for axis, length in enumerate(result.shape)]
    widest = result.shape.index(max(result.shape))
    beside = place[:widest] + [(place[widest] + 1) % result.shape[widest]] + place[widest + 1:]
    return result.at[tuple(place)].set(least).at[tuple(beside)].set(largest)


def level_of(rng, shape, pieces, low, largest):
    def one(dim, parts):
        steps = jax.random.uniform(jax.random.fold_in(jax.random.fold_in(rng, 6), dim), (parts,), jnp.float32, low / len(pieces), largest / len(pieces))
        return jnp.repeat(jnp.exp(steps), shape[dim] // parts).reshape((-1,) + (1,) * (len(shape) - dim - 1))

    loudness = one(*pieces[0])
    for cut in pieces[1:]:
        loudness = loudness * one(*cut)
    return loudness


def bell_draw(stream_key, extent, scale, reach, pieces=(), kind=jnp.bfloat16):
    drawn = jax.random.normal(stream_key, extent, jnp.float32) * scale
    if len(pieces) > 0:
        drawn = level_of(stream_key, extent, pieces, -0.22, 0.18) * drawn
    return jnp.clip(drawn, min=-reach, max=reach).astype(kind)


def setup_inputs(seed: int = 0) -> dict:
    arg_keys = jax.random.split(jax.random.key(seed), 7)
    rewards = bell_draw(arg_keys[0], (TIME, ENVS), 1.0, 6.0, ((0, 4), (1, 8)), jnp.float32)
    dones = place_ends((jax.random.randint(arg_keys[1], (TIME, ENVS), 0, 4 * TIME) < 1).astype(jnp.int32), jax.random.fold_in(arg_keys[1], 1), 0, 1)
    horizon = jnp.clip(jnp.exp(math.log(2048.0) - 4.6288867 * jax.random.uniform(arg_keys[2], (ENVS,), jnp.float32) ** level_of(arg_keys[2], (ENVS,), ((0, 8),), -0.2, 0.2)), 20.0, 2048.0)
    bootstrap = bell_draw(arg_keys[3], (ENVS,), 16.0, 96.0, ((0, 8),), jnp.float32)
    prior_mean = bell_draw(arg_keys[4], (1,), 40.0, 240.0, (), jnp.float32)
    prior_var = jnp.clip(jnp.exp(jax.random.uniform(arg_keys[5], (1,), jnp.float32, math.log(100.0), math.log(3000.0))), 100.0, 3000.0)
    return {"rewards": rewards, "dones": dones, "horizon": horizon, "bootstrap": bootstrap, "prior_mean": prior_mean, "prior_var": prior_var}


def reference(rewards, dones, horizon, bootstrap, prior_mean, prior_var):
    discount = 1.0 - 1.0 / horizon
    factor = discount[None, :] * (1.0 - dones.astype(jnp.float32))

    def backward(carried, inputs):
        reward_row, factor_row = inputs
        updated = reward_row + factor_row * carried
        return (updated, updated)
    final_carry, returns = lax.scan(backward, bootstrap, (rewards, factor), reverse=True)
    entries = jnp.float32(returns.size)
    average = jnp.sum(returns) / entries
    spread = jnp.sum((returns - average) * (returns - average))
    prior_count = jnp.float32(PRIOR)
    merged = prior_count + entries
    delta = average - prior_mean[0]
    new_mean = prior_mean[0] + delta * entries / merged
    new_spread = prior_var[0] * prior_count + spread + delta * delta * prior_count * entries / merged
    variance = new_spread / merged
    inverse = 1.0 / jnp.sqrt(variance + 1e-08)
    return (rewards * inverse, returns * inverse, jnp.stack([new_mean, variance]))
```

```python
import functools

import jax
import jax.numpy as jnp
from jax import lax
from jax.experimental import pallas as pl
from jax.experimental.pallas import tpu as pltpu
from jax.sharding import PartitionSpec as P

SUB = 8
ROWS = 8


def compose_rows(summed, product, row):
    step = 1
    while step < SUB:
        inside = row < SUB - step
        later_sum = jnp.where(inside, pltpu.roll(summed, SUB - step, 0), 0.0)
        later_product = jnp.where(inside, pltpu.roll(product, SUB - step, 0), 1.0)
        summed = summed + product * later_sum
        product = product * later_product
        step *= 2
    return summed, product


def kernel(T, E, rewards_hbm, dones_hbm, horizon_ref, bootstrap_ref, mean_ref, var_ref,
           returns_ref, inverse_ref, stats_ref,
           rewards, dones, s_buf, p_buf, tbuf, ebuf, load_sem, tsend, trecv, esend, erecv):
    t = lax.axis_index("tm")
    e = lax.axis_index("env")
    barrier = pltpu.get_barrier_semaphore()
    for d in range(1, T):
        pl.semaphore_signal(barrier, inc=1, device_id={"tm": lax.rem(t + d, T)},
                            device_id_type=pl.DeviceIdType.MESH)
    for d in range(1, E):
        pl.semaphore_signal(barrier, inc=1, device_id={"env": lax.rem(e + d, E)},
                            device_id_type=pl.DeviceIdType.MESH)
    loads = [pltpu.make_async_copy(rewards_hbm, rewards, load_sem.at[0]),
             pltpu.make_async_copy(dones_hbm, dones, load_sem.at[1])]
    for load in loads:
        load.start()
    rows, lanes = rewards.shape
    chunk = rows // SUB
    shape = (SUB, lanes)
    row = lax.broadcasted_iota(jnp.int32, shape, 0)
    discount = jnp.broadcast_to(1.0 - 1.0 / horizon_ref[...], shape)
    center = jnp.broadcast_to(mean_ref[...], shape)
    for load in loads:
        load.wait()
    s = jnp.zeros(shape, jnp.float32)
    p = jnp.ones(shape, jnp.float32)
    zero = jnp.zeros(shape, jnp.float32)
    s1, p1, s2, sp, p2 = zero, zero, zero, zero, zero
    for k in reversed(range(chunk)):
        r = rewards[pl.ds(k, SUB, stride=chunk), :]
        f = jnp.where(dones[pl.ds(k, SUB, stride=chunk), :] == 0, discount, 0.0)
        s = r + f * s
        p = f * p
        s_buf[k] = s
        p_buf[k] = p
        c = s - center
        s1 = s1 + c
        p1 = p1 + p
        s2 = s2 + c * c
        sp = sp + c * p
        p2 = p2 + p * p
    full_s, full_p = compose_rows(s, p, row)
    last = row == SUB - 1
    a = jnp.where(last, 0.0, pltpu.roll(full_s, SUB - 1, 0))
    b = jnp.where(last, 1.0, pltpu.roll(full_p, SUB - 1, 0))
    down = lambda value: jnp.sum(value, axis=0, keepdims=True)
    tbuf[t, 0:1] = full_s[0:1]
    tbuf[t, 1:2] = full_p[0:1]
    tbuf[t, 2:3] = down(s1 + p1 * a)
    tbuf[t, 3:4] = down(p1 * b)
    tbuf[t, 4:5] = down(s2 + a * (2.0 * sp + a * p2))
    tbuf[t, 5:6] = down(2.0 * b * (sp + a * p2))
    tbuf[t, 6:7] = down(b * b * p2)
    tbuf[t, 7:8] = jnp.zeros((1, lanes), jnp.float32)
    pl.semaphore_wait(barrier, T + E - 2)
    copies = []
    for d in range(1, T):
        copies.append(pltpu.make_async_remote_copy(
            tbuf.at[t], tbuf.at[t], tsend.at[d - 1], trecv.at[d - 1],
            device_id={"tm": lax.rem(t + d, T)}, device_id_type=pl.DeviceIdType.MESH))
    for copy in copies:
        copy.start()
    for copy in copies:
        copy.wait()
    x = bootstrap_ref[...]
    mine = x
    first = jnp.zeros((1, lanes), jnp.float32)
    second = jnp.zeros((1, lanes), jnp.float32)
    for j in reversed(range(T)):
        mine = jnp.where(t == j, x, mine)
        first = first + tbuf[j, 2:3] + tbuf[j, 3:4] * x
        second = second + tbuf[j, 4:5] + x * (tbuf[j, 5:6] + x * tbuf[j, 6:7])
        x = tbuf[j, 0:1] + tbuf[j, 1:2] * x
    ebuf[e, 0:1] = first
    ebuf[e, 1:2] = second
    copies = []
    for d in range(1, E):
        copies.append(pltpu.make_async_remote_copy(
            ebuf.at[e], ebuf.at[e], esend.at[d - 1], erecv.at[d - 1],
            device_id={"env": lax.rem(e + d, E)}, device_id_type=pl.DeviceIdType.MESH))
    for copy in copies:
        copy.start()
    y = a + b * mine
    for k in range(chunk):
        returns_ref[pl.ds(k, SUB, stride=chunk), :] = s_buf[k] + p_buf[k] * y
    for copy in copies:
        copy.wait()
    total = ebuf[0]
    for j in range(1, E):
        total = total + ebuf[j]
    sums = jnp.sum(total, axis=1, keepdims=True)
    entries = jnp.float32(rows * T * lanes * E)
    first = sums[0:1]
    second = sums[1:2]
    mean0 = mean_ref[...]
    average = mean0 + first / entries
    spread = second - first * first / entries
    prior_count = entries
    merged = prior_count + entries
    delta = average - mean0
    new_mean = mean0 + delta * entries / merged
    new_spread = var_ref[...] * prior_count + spread + delta * delta * prior_count * entries / merged
    variance = new_spread / merged
    inverse_ref[...] = jnp.broadcast_to(1.0 / jnp.sqrt(variance + 1e-08), inverse_ref.shape)
    lane = lax.broadcasted_iota(jnp.int32, (1, lanes), 1)
    stats_ref[...] = jnp.where(lane == 0, new_mean, variance)


def local(T, E, rewards, dones, horizon, bootstrap, prior_mean, prior_var):
    rows, lanes = rewards.shape
    vmem = pl.BlockSpec(memory_space=pltpu.VMEM)
    hbm = pl.BlockSpec(memory_space=pl.ANY)
    returns, inverse, stats = pl.pallas_call(
        functools.partial(kernel, T, E),
        out_shape=(jax.ShapeDtypeStruct((rows, lanes), jnp.float32),
                   jax.ShapeDtypeStruct((1, lanes), jnp.float32),
                   jax.ShapeDtypeStruct((1, lanes), jnp.float32)),
        in_specs=[hbm, hbm, vmem, vmem, vmem, vmem],
        out_specs=(vmem, vmem, vmem),
        scratch_shapes=[
            pltpu.VMEM((rows, lanes), jnp.float32),
            pltpu.VMEM((rows, lanes), jnp.int32),
            pltpu.VMEM((rows // SUB, SUB, lanes), jnp.float32),
            pltpu.VMEM((rows // SUB, SUB, lanes), jnp.float32),
            pltpu.VMEM((T, ROWS, lanes), jnp.float32),
            pltpu.VMEM((E, 2, lanes), jnp.float32),
            pltpu.SemaphoreType.DMA((2,)),
            pltpu.SemaphoreType.DMA((T - 1,)),
            pltpu.SemaphoreType.DMA((T - 1,)),
            pltpu.SemaphoreType.DMA((E - 1,)),
            pltpu.SemaphoreType.DMA((E - 1,)),
        ],
        compiler_params=pltpu.CompilerParams(collective_id=0, has_side_effects=True),
    )(rewards, dones, horizon.reshape(1, lanes), bootstrap.reshape(1, lanes),
      prior_mean.reshape(1, 1), prior_var.reshape(1, 1))
    return (rewards * inverse, returns * inverse, stats[0, :2])


def solution(mesh):
    T, E = mesh.shape["tm"], mesh.shape["env"]
    return jax.shard_map(
        functools.partial(local, T, E),
        mesh=mesh,
        in_specs=(P("tm", "env"), P("tm", "env"), P("env"), P("env"), P(), P()),
        out_specs=(P("tm", "env"), P("tm", "env"), P()),
        check_vma=False,
    )
```

```python
import functools

import jax
import jax.numpy as jnp
from jax import lax
from jax.experimental import pallas as pl
from jax.experimental.pallas import tpu as pltpu
from jax.sharding import PartitionSpec as P

SUB = 8
ROWS = 8
PARTS = 4


def compose_rows(summed, product, row):
    step = 1
    while step < SUB:
        inside = row < SUB - step
        later_sum = jnp.where(inside, pltpu.roll(summed, SUB - step, 0), 0.0)
        later_product = jnp.where(inside, pltpu.roll(product, SUB - step, 0), 1.0)
        summed = summed + product * later_sum
        product = product * later_product
        step *= 2
    return summed, product


def kernel(T, E, rewards_hbm, dones_hbm, horizon_hbm, bootstrap_hbm, mean_hbm, var_hbm,
           rewards, returns_ref, ebuf, prior_ref,
           dones, horizon_ref, bootstrap_ref, mean_ref, var_ref, s_buf, p_buf, tbuf,
           load_sem, tsend, trecv, esend, erecv):
    t = lax.axis_index("tm")
    e = lax.axis_index("env")
    barrier = pltpu.get_barrier_semaphore()
    for d in range(1, T):
        pl.semaphore_signal(barrier, inc=1, device_id={"tm": lax.rem(t + d, T)},
                            device_id_type=pl.DeviceIdType.MESH)
    for d in range(1, E):
        pl.semaphore_signal(barrier, inc=1, device_id={"env": lax.rem(e + d, E)},
                            device_id_type=pl.DeviceIdType.MESH)
    pairs = [(horizon_hbm, horizon_ref), (mean_hbm, mean_ref), (var_hbm, var_ref),
             (bootstrap_hbm, bootstrap_ref), (rewards_hbm, rewards),
             (dones_hbm, dones)]
    loads = [pltpu.make_async_copy(source, target, load_sem.at[i])
             for i, (source, target) in enumerate(pairs)]
    for load in loads:
        load.start()
    rows, lanes = rewards.shape
    chunk = rows // SUB
    shape = (SUB, lanes)
    row = lax.broadcasted_iota(jnp.int32, shape, 0)
    for load in loads:
        load.wait()
    discount = jnp.broadcast_to(1.0 - 1.0 / horizon_ref[...], shape)
    center = jnp.full(shape, mean_ref[0], jnp.float32)
    s = jnp.zeros(shape, jnp.float32)
    p = jnp.ones(shape, jnp.float32)
    zero = jnp.zeros(shape, jnp.float32)
    s1, p1, s2, sp, p2 = zero, zero, zero, zero, zero
    for k in reversed(range(chunk)):
        r = rewards[pl.ds(k, SUB, stride=chunk), :]
        f = jnp.where(dones[pl.ds(k, SUB, stride=chunk), :] == 0, discount, 0.0)
        s = r + f * s
        p = f * p
        s_buf[k] = s
        p_buf[k] = p
        c = s - center
        s1 = s1 + c
        p1 = p1 + p
        s2 = s2 + c * c
        sp = sp + c * p
        p2 = p2 + p * p
    full_s, full_p = compose_rows(s, p, row)
    last = row == SUB - 1
    a = jnp.where(last, 0.0, pltpu.roll(full_s, SUB - 1, 0))
    b = jnp.where(last, 1.0, pltpu.roll(full_p, SUB - 1, 0))
    down = lambda value: jnp.sum(value, axis=0, keepdims=True)
    tbuf[t, 0:1] = full_s[0:1]
    tbuf[t, 1:2] = full_p[0:1]
    tbuf[t, 2:3] = down(s1 + p1 * a)
    tbuf[t, 3:4] = down(p1 * b)
    tbuf[t, 4:5] = down(s2 + a * (2.0 * sp + a * p2))
    tbuf[t, 5:6] = down(2.0 * b * (sp + a * p2))
    tbuf[t, 6:7] = down(b * b * p2)
    tbuf[t, 7:8] = jnp.zeros((1, lanes), jnp.float32)
    pl.semaphore_wait(barrier, T + E - 2)
    copies = []
    for d in range(1, T):
        copies.append(pltpu.make_async_remote_copy(
            tbuf.at[t], tbuf.at[t], tsend.at[d - 1], trecv.at[d - 1],
            device_id={"tm": lax.rem(t + d, T)}, device_id_type=pl.DeviceIdType.MESH))
    for copy in copies:
        copy.start()
    for copy in copies:
        copy.wait()
    x = bootstrap_ref[...]
    mine = x
    first = jnp.zeros((1, lanes), jnp.float32)
    second = jnp.zeros((1, lanes), jnp.float32)
    for j in reversed(range(T)):
        mine = jnp.where(t == j, x, mine)
        first = first + tbuf[j, 2:3] + tbuf[j, 3:4] * x
        second = second + tbuf[j, 4:5] + x * (tbuf[j, 5:6] + x * tbuf[j, 6:7])
        x = tbuf[j, 0:1] + tbuf[j, 1:2] * x
    ebuf[e, 0:1] = first
    ebuf[e, 1:2] = second
    copies = []
    for d in range(1, E):
        copies.append(pltpu.make_async_remote_copy(
            ebuf.at[e], ebuf.at[e], esend.at[d - 1], erecv.at[d - 1],
            device_id={"env": lax.rem(e + d, E)}, device_id_type=pl.DeviceIdType.MESH))
    for copy in copies:
        copy.start()
    prior_ref[0:1] = center[0:1]
    prior_ref[1:2] = jnp.full((1, lanes), var_ref[0], jnp.float32)
    y = a + b * mine
    for k in range(chunk):
        returns_ref[pl.ds(k, SUB, stride=chunk), :] = s_buf[k] + p_buf[k] * y
    for copy in copies:
        copy.wait()


def finish(T, E, rewards, returns, ebuf, prior_ref, out_rewards, out_returns, stats_ref,
           rewards_out, returns_out, sems):
    rows, lanes = rewards.shape
    total = ebuf[0]
    for j in range(1, E):
        total = total + ebuf[j]
    sums = jnp.sum(total, axis=1, keepdims=True)
    entries = jnp.float32(rows * T * lanes * E)
    first = sums[0:1]
    second = sums[1:2]
    mean0 = prior_ref[0:1, 0:1]
    var0 = prior_ref[1:2, 0:1]
    average = mean0 + first / entries
    spread = second - first * first / entries
    prior_count = entries
    merged = prior_count + entries
    delta = average - mean0
    new_mean = mean0 + delta * entries / merged
    new_spread = var0 * prior_count + spread + delta * delta * prior_count * entries / merged
    variance = new_spread / merged
    inverse = jnp.broadcast_to(1.0 / jnp.sqrt(variance + 1e-08), (SUB, lanes))
    copies = []
    part = rows // PARTS
    for i in range(PARTS):
        for n, (source, staged, target) in enumerate(
                ((rewards, rewards_out, out_rewards), (returns, returns_out, out_returns))):
            for k in range(i * part, (i + 1) * part, SUB):
                staged[k:k + SUB] = source[k:k + SUB] * inverse
            where = pl.ds(i * part, part)
            copy = pltpu.make_async_copy(staged.at[where], target.at[where], sems.at[n, i])
            copy.start()
            copies.append(copy)
    stats_ref[0] = new_mean[0, 0]
    stats_ref[1] = variance[0, 0]
    for copy in copies:
        copy.wait()


def local(T, E, rewards, dones, horizon, bootstrap, prior_mean, prior_var):
    rows, lanes = rewards.shape
    block = (rows, lanes)
    vmem = pl.BlockSpec(memory_space=pltpu.VMEM)
    smem = pl.BlockSpec(memory_space=pltpu.SMEM)
    hbm = pl.BlockSpec(memory_space=pltpu.HBM)
    kept, returns, sums, prior = pl.pallas_call(
        functools.partial(kernel, T, E),
        out_shape=(pltpu.VMEM(block, jnp.float32), pltpu.VMEM(block, jnp.float32),
                   pltpu.VMEM((E, 2, lanes), jnp.float32), pltpu.VMEM((2, lanes), jnp.float32)),
        in_specs=[hbm] * 6,
        out_specs=(vmem, vmem, vmem, vmem),
        scratch_shapes=[
            pltpu.VMEM(block, jnp.int32),
            pltpu.VMEM((1, lanes), jnp.float32),
            pltpu.VMEM((1, lanes), jnp.float32),
            pltpu.SMEM((1,), jnp.float32),
            pltpu.SMEM((1,), jnp.float32),
            pltpu.VMEM((rows // SUB, SUB, lanes), jnp.float32),
            pltpu.VMEM((rows // SUB, SUB, lanes), jnp.float32),
            pltpu.VMEM((T, ROWS, lanes), jnp.float32),
            pltpu.SemaphoreType.DMA((6,)),
            pltpu.SemaphoreType.DMA((T - 1,)),
            pltpu.SemaphoreType.DMA((T - 1,)),
            pltpu.SemaphoreType.DMA((E - 1,)),
            pltpu.SemaphoreType.DMA((E - 1,)),
        ],
        compiler_params=pltpu.CompilerParams(collective_id=0, has_side_effects=True),
    )(rewards, dones, horizon.reshape(1, lanes), bootstrap.reshape(1, lanes), prior_mean, prior_var)
    return pl.pallas_call(
        functools.partial(finish, T, E),
        out_shape=(jax.ShapeDtypeStruct(block, jnp.float32),
                   jax.ShapeDtypeStruct(block, jnp.float32),
                   jax.ShapeDtypeStruct((2,), jnp.float32)),
        in_specs=[vmem] * 4,
        out_specs=(hbm, hbm, smem),
        scratch_shapes=[
            pltpu.VMEM(block, jnp.float32),
            pltpu.VMEM(block, jnp.float32),
            pltpu.SemaphoreType.DMA((2, PARTS)),
        ],
        compiler_params=pltpu.CompilerParams(vmem_limit_bytes=4 * 2**20),
    )(kept, returns, sums, prior)


def solution(mesh):
    T, E = mesh.shape["tm"], mesh.shape["env"]
    return jax.shard_map(
        functools.partial(local, T, E),
        mesh=mesh,
        in_specs=(P("tm", "env"), P("tm", "env"), P("env"), P("env"), P(), P()),
        out_specs=(P("tm", "env"), P("tm", "env"), P()),
        check_vma=False,
    )
```

```python
import functools

import jax
import jax.numpy as jnp
from jax import lax
from jax.experimental import pallas as pl
from jax.experimental.pallas import tpu as pltpu
from jax.sharding import PartitionSpec as P

SUB = 8
ROWS = 8
PARTS = 4


def compose_rows(summed, product, row):
    step = 1
    while step < SUB:
        inside = row < SUB - step
        later_sum = jnp.where(inside, pltpu.roll(summed, SUB - step, 0), 0.0)
        later_product = jnp.where(inside, pltpu.roll(product, SUB - step, 0), 1.0)
        summed = summed + product * later_sum
        product = product * later_product
        step *= 2
    return summed, product


def kernel(T, E, rewards_hbm, dones_hbm, horizon_hbm, bootstrap_hbm, prior_hbm,
           rewards, returns_ref, ebuf, prior_ref,
           dones, horizon_ref, bootstrap_ref, s_buf, p_buf, tbuf,
           load_sem, tsend, trecv, esend, erecv):
    t = lax.axis_index("tm")
    e = lax.axis_index("env")
    barrier = pltpu.get_barrier_semaphore()
    for d in range(1, T):
        pl.semaphore_signal(barrier, inc=1, device_id={"tm": lax.rem(t + d, T)},
                            device_id_type=pl.DeviceIdType.MESH)
    for d in range(1, E):
        pl.semaphore_signal(barrier, inc=1, device_id={"env": lax.rem(e + d, E)},
                            device_id_type=pl.DeviceIdType.MESH)
    pairs = [(horizon_hbm, horizon_ref), (prior_hbm, prior_ref),
             (bootstrap_hbm, bootstrap_ref), (rewards_hbm, rewards),
             (dones_hbm, dones)]
    loads = [pltpu.make_async_copy(source, target, load_sem.at[i])
             for i, (source, target) in enumerate(pairs)]
    for load in loads:
        load.start()
    rows, lanes = rewards.shape
    chunk = rows // SUB
    shape = (SUB, lanes)
    row = lax.broadcasted_iota(jnp.int32, shape, 0)
    for load in loads:
        load.wait()
    discount = jnp.broadcast_to(1.0 - 1.0 / horizon_ref[...], shape)
    center = jnp.broadcast_to(prior_ref[0:1], shape)
    s = jnp.zeros(shape, jnp.float32)
    p = jnp.ones(shape, jnp.float32)
    zero = jnp.zeros(shape, jnp.float32)
    s1, p1, s2, sp, p2 = zero, zero, zero, zero, zero
    for k in reversed(range(chunk)):
        r = rewards[pl.ds(k, SUB, stride=chunk), :]
        f = jnp.where(dones[pl.ds(k, SUB, stride=chunk), :] == 0, discount, 0.0)
        s = r + f * s
        p = f * p
        s_buf[k] = s
        p_buf[k] = p
        c = s - center
        s1 = s1 + c
        p1 = p1 + p
        s2 = s2 + c * c
        sp = sp + c * p
        p2 = p2 + p * p
    full_s, full_p = compose_rows(s, p, row)
    last = row == SUB - 1
    a = jnp.where(last, 0.0, pltpu.roll(full_s, SUB - 1, 0))
    b = jnp.where(last, 1.0, pltpu.roll(full_p, SUB - 1, 0))
    down = lambda value: jnp.sum(value, axis=0, keepdims=True)
    tbuf[t, 0:1] = full_s[0:1]
    tbuf[t, 1:2] = full_p[0:1]
    tbuf[t, 2:3] = down(s1 + p1 * a)
    tbuf[t, 3:4] = down(p1 * b)
    tbuf[t, 4:5] = down(s2 + a * (2.0 * sp + a * p2))
    tbuf[t, 5:6] = down(2.0 * b * (sp + a * p2))
    tbuf[t, 6:7] = down(b * b * p2)
    tbuf[t, 7:8] = jnp.zeros((1, lanes), jnp.float32)
    pl.semaphore_wait(barrier, T + E - 2)
    copies = []
    for d in range(1, T):
        copies.append(pltpu.make_async_remote_copy(
            tbuf.at[t], tbuf.at[t], tsend.at[d - 1], trecv.at[d - 1],
            device_id={"tm": lax.rem(t + d, T)}, device_id_type=pl.DeviceIdType.MESH))
    for copy in copies:
        copy.start()
    for copy in copies:
        copy.wait()
    x = bootstrap_ref[...]
    mine = x
    first = jnp.zeros((1, lanes), jnp.float32)
    second = jnp.zeros((1, lanes), jnp.float32)
    for j in reversed(range(T)):
        mine = jnp.where(t == j, x, mine)
        first = first + tbuf[j, 2:3] + tbuf[j, 3:4] * x
        second = second + tbuf[j, 4:5] + x * (tbuf[j, 5:6] + x * tbuf[j, 6:7])
        x = tbuf[j, 0:1] + tbuf[j, 1:2] * x
    ebuf[e, 0:1] = first
    ebuf[e, 1:2] = second
    copies = []
    for d in range(1, E):
        copies.append(pltpu.make_async_remote_copy(
            ebuf.at[e], ebuf.at[e], esend.at[d - 1], erecv.at[d - 1],
            device_id={"env": lax.rem(e + d, E)}, device_id_type=pl.DeviceIdType.MESH))
    for copy in copies:
        copy.start()
    y = a + b * mine
    for k in range(chunk):
        returns_ref[pl.ds(k, SUB, stride=chunk), :] = s_buf[k] + p_buf[k] * y
    for copy in copies:
        copy.wait()


def finish(T, E, rewards, returns, ebuf, prior_ref, out_rewards, out_returns, stats_ref,
           rewards_out, returns_out, sems):
    rows, lanes = rewards.shape
    total = ebuf[0]
    for j in range(1, E):
        total = total + ebuf[j]
    sums = jnp.sum(total, axis=1, keepdims=True)
    entries = jnp.float32(rows * T * lanes * E)
    first = sums[0:1]
    second = sums[1:2]
    mean0 = prior_ref[0:1, 0:1]
    var0 = prior_ref[1:2, 0:1]
    average = mean0 + first / entries
    spread = second - first * first / entries
    prior_count = entries
    merged = prior_count + entries
    delta = average - mean0
    new_mean = mean0 + delta * entries / merged
    new_spread = var0 * prior_count + spread + delta * delta * prior_count * entries / merged
    variance = new_spread / merged
    inverse = jnp.broadcast_to(1.0 / jnp.sqrt(variance + 1e-08), (SUB, lanes))
    copies = []
    part = rows // PARTS
    for i in range(PARTS):
        for n, (source, staged, target) in enumerate(
                ((rewards, rewards_out, out_rewards), (returns, returns_out, out_returns))):
            for k in range(i * part, (i + 1) * part, SUB):
                staged[k:k + SUB] = source[k:k + SUB] * inverse
            where = pl.ds(i * part, part)
            copy = pltpu.make_async_copy(staged.at[where], target.at[where], sems.at[n, i])
            copy.start()
            copies.append(copy)
    stats_ref[0] = new_mean[0, 0]
    stats_ref[1] = variance[0, 0]
    for copy in copies:
        copy.wait()


def local(T, E, rewards, dones, horizon, bootstrap, prior_mean, prior_var):
    rows, lanes = rewards.shape
    block = (rows, lanes)
    vmem = pl.BlockSpec(memory_space=pltpu.VMEM)
    smem = pl.BlockSpec(memory_space=pltpu.SMEM)
    hbm = pl.BlockSpec(memory_space=pltpu.HBM)
    row = lax.broadcasted_iota(jnp.int32, (2, lanes), 0)
    prior = jnp.where(row == 0, prior_mean, prior_var)
    kept, returns, sums, prior = pl.pallas_call(
        functools.partial(kernel, T, E),
        out_shape=(pltpu.VMEM(block, jnp.float32), pltpu.VMEM(block, jnp.float32),
                   pltpu.VMEM((E, 2, lanes), jnp.float32), pltpu.VMEM((2, lanes), jnp.float32)),
        in_specs=[hbm] * 5,
        out_specs=(vmem, vmem, vmem, vmem),
        scratch_shapes=[
            pltpu.VMEM(block, jnp.int32),
            pltpu.VMEM((1, lanes), jnp.float32),
            pltpu.VMEM((1, lanes), jnp.float32),
            pltpu.VMEM((rows // SUB, SUB, lanes), jnp.float32),
            pltpu.VMEM((rows // SUB, SUB, lanes), jnp.float32),
            pltpu.VMEM((T, ROWS, lanes), jnp.float32),
            pltpu.SemaphoreType.DMA((5,)),
            pltpu.SemaphoreType.DMA((T - 1,)),
            pltpu.SemaphoreType.DMA((T - 1,)),
            pltpu.SemaphoreType.DMA((E - 1,)),
            pltpu.SemaphoreType.DMA((E - 1,)),
        ],
        compiler_params=pltpu.CompilerParams(collective_id=0, has_side_effects=True),
    )(rewards, dones, horizon.reshape(1, lanes), bootstrap.reshape(1, lanes), prior)
    return pl.pallas_call(
        functools.partial(finish, T, E),
        out_shape=(jax.ShapeDtypeStruct(block, jnp.float32),
                   jax.ShapeDtypeStruct(block, jnp.float32),
                   jax.ShapeDtypeStruct((2,), jnp.float32)),
        in_specs=[vmem] * 4,
        out_specs=(hbm, hbm, smem),
        scratch_shapes=[
            pltpu.VMEM(block, jnp.float32),
            pltpu.VMEM(block, jnp.float32),
            pltpu.SemaphoreType.DMA((2, PARTS)),
        ],
        compiler_params=pltpu.CompilerParams(vmem_limit_bytes=4 * 2**20),
    )(kept, returns, sums, prior)


def solution(mesh):
    T, E = mesh.shape["tm"], mesh.shape["env"]
    return jax.shard_map(
        functools.partial(local, T, E),
        mesh=mesh,
        in_specs=(P("tm", "env"), P("tm", "env"), P("env"), P("env"), P(), P()),
        out_specs=(P("tm", "env"), P("tm", "env"), P()),
        check_vma=False,
    )
```

```python
import functools

import jax
import jax.numpy as jnp
from jax import lax
from jax.experimental import pallas as pl
from jax.experimental.pallas import tpu as pltpu
from jax.sharding import PartitionSpec as P

SUB = 8
ROWS = 8
PARTS = 4


def compose_rows(summed, product, row):
    step = 1
    while step < SUB:
        inside = row < SUB - step
        later_sum = jnp.where(inside, pltpu.roll(summed, SUB - step, 0), 0.0)
        later_product = jnp.where(inside, pltpu.roll(product, SUB - step, 0), 1.0)
        summed = summed + product * later_sum
        product = product * later_product
        step *= 2
    return summed, product


def kernel(T, E, rewards_hbm, dones_hbm, horizon_hbm, bootstrap_hbm, mean_hbm, var_hbm,
           rewards, returns_ref, ebuf, prior_ref,
           dones, horizon_ref, bootstrap_ref, mean_ref, var_ref, s_buf, p_buf, tbuf, xbuf,
           load_sem, tsend, trecv):
    t = lax.axis_index("tm")
    e = lax.axis_index("env")
    barrier = pltpu.get_barrier_semaphore()
    offsets = [(i, j) for i in range(T) for j in range(E) if i or j]
    offsets.sort(key=lambda o: -min(o[0], T - o[0]))
    peers = [{"tm": lax.rem(t + i, T), "env": lax.rem(e + j, E)} for i, j in offsets]
    for peer in peers:
        pl.semaphore_signal(barrier, inc=1, device_id=peer, device_id_type=pl.DeviceIdType.MESH)
    pairs = [(horizon_hbm, horizon_ref), (mean_hbm, mean_ref), (var_hbm, var_ref),
             (bootstrap_hbm, bootstrap_ref), (rewards_hbm, rewards),
             (dones_hbm, dones)]
    loads = [pltpu.make_async_copy(source, target, load_sem.at[i])
             for i, (source, target) in enumerate(pairs)]
    for load in loads:
        load.start()
    rows, lanes = rewards.shape
    chunk = rows // SUB
    shape = (SUB, lanes)
    row = lax.broadcasted_iota(jnp.int32, shape, 0)
    for load in loads:
        load.wait()
    discount = jnp.broadcast_to(1.0 - 1.0 / horizon_ref[...], shape)
    center = jnp.full(shape, mean_ref[0], jnp.float32)
    s = jnp.zeros(shape, jnp.float32)
    p = jnp.ones(shape, jnp.float32)
    zero = jnp.zeros(shape, jnp.float32)
    s1, p1, s2, sp, p2 = zero, zero, zero, zero, zero
    for k in reversed(range(chunk)):
        r = rewards[pl.ds(k, SUB, stride=chunk), :]
        f = jnp.where(dones[pl.ds(k, SUB, stride=chunk), :] == 0, discount, 0.0)
        s = r + f * s
        p = f * p
        s_buf[k] = s
        p_buf[k] = p
        c = s - center
        s1 = s1 + c
        p1 = p1 + p
        s2 = s2 + c * c
        sp = sp + c * p
        p2 = p2 + p * p
    full_s, full_p = compose_rows(s, p, row)
    last = row == SUB - 1
    a = jnp.where(last, 0.0, pltpu.roll(full_s, SUB - 1, 0))
    b = jnp.where(last, 1.0, pltpu.roll(full_p, SUB - 1, 0))
    down = lambda value: jnp.sum(value, axis=0, keepdims=True)
    tbuf[t, e, 0:1] = full_s[0:1]
    tbuf[t, e, 1:2] = full_p[0:1]
    tbuf[t, e, 2:3] = down(s1 + p1 * a)
    tbuf[t, e, 3:4] = down(p1 * b)
    tbuf[t, e, 4:5] = down(s2 + a * (2.0 * sp + a * p2))
    tbuf[t, e, 5:6] = down(2.0 * b * (sp + a * p2))
    tbuf[t, e, 6:7] = down(b * b * p2)
    tbuf[t, e, 7:8] = bootstrap_ref[...]
    pl.semaphore_wait(barrier, T * E - 1)
    copies = [pltpu.make_async_remote_copy(
        tbuf.at[t, e], tbuf.at[t, e], tsend.at[i], trecv.at[i],
        device_id=peer, device_id_type=pl.DeviceIdType.MESH) for i, peer in enumerate(peers)]
    for copy in copies:
        copy.start()
    for copy in copies:
        copy.wait()
    x = tbuf[T - 1, :, 7]
    first = jnp.zeros((E, lanes), jnp.float32)
    second = jnp.zeros((E, lanes), jnp.float32)
    for j in reversed(range(T)):
        xbuf[j] = x
        first = first + tbuf[j, :, 2] + tbuf[j, :, 3] * x
        second = second + tbuf[j, :, 4] + x * (tbuf[j, :, 5] + x * tbuf[j, :, 6])
        x = tbuf[j, :, 0] + tbuf[j, :, 1] * x
    mine = xbuf[t, pl.ds(e, 1), :]
    ebuf[0] = first
    ebuf[1] = second
    prior_ref[0:1] = center[0:1]
    prior_ref[1:2] = jnp.full((1, lanes), var_ref[0], jnp.float32)
    y = a + b * mine
    for k in range(chunk):
        returns_ref[pl.ds(k, SUB, stride=chunk), :] = s_buf[k] + p_buf[k] * y


def finish(T, E, rewards, returns, ebuf, prior_ref, out_rewards, out_returns, stats_ref,
           rewards_out, returns_out, sems):
    rows, lanes = rewards.shape
    first = jnp.sum(jnp.sum(ebuf[0], axis=0, keepdims=True), axis=1, keepdims=True)
    second = jnp.sum(jnp.sum(ebuf[1], axis=0, keepdims=True), axis=1, keepdims=True)
    entries = jnp.float32(rows * T * lanes * E)
    mean0 = prior_ref[0:1, 0:1]
    var0 = prior_ref[1:2, 0:1]
    average = mean0 + first / entries
    spread = second - first * first / entries
    prior_count = entries
    merged = prior_count + entries
    delta = average - mean0
    new_mean = mean0 + delta * entries / merged
    new_spread = var0 * prior_count + spread + delta * delta * prior_count * entries / merged
    variance = new_spread / merged
    inverse = jnp.broadcast_to(1.0 / jnp.sqrt(variance + 1e-08), (SUB, lanes))
    copies = []
    part = rows // PARTS
    for i in range(PARTS):
        for n, (source, staged, target) in enumerate(
                ((rewards, rewards_out, out_rewards), (returns, returns_out, out_returns))):
            for k in range(i * part, (i + 1) * part, SUB):
                staged[k:k + SUB] = source[k:k + SUB] * inverse
            where = pl.ds(i * part, part)
            copy = pltpu.make_async_copy(staged.at[where], target.at[where], sems.at[n, i])
            copy.start()
            copies.append(copy)
    stats_ref[0] = new_mean[0, 0]
    stats_ref[1] = variance[0, 0]
    for copy in copies:
        copy.wait()


def local(T, E, rewards, dones, horizon, bootstrap, prior_mean, prior_var):
    rows, lanes = rewards.shape
    block = (rows, lanes)
    vmem = pl.BlockSpec(memory_space=pltpu.VMEM)
    smem = pl.BlockSpec(memory_space=pltpu.SMEM)
    hbm = pl.BlockSpec(memory_space=pltpu.HBM)
    kept, returns, sums, prior = pl.pallas_call(
        functools.partial(kernel, T, E),
        out_shape=(pltpu.VMEM(block, jnp.float32), pltpu.VMEM(block, jnp.float32),
                   pltpu.VMEM((2, E, lanes), jnp.float32), pltpu.VMEM((2, lanes), jnp.float32)),
        in_specs=[hbm] * 6,
        out_specs=(vmem, vmem, vmem, vmem),
        scratch_shapes=[
            pltpu.VMEM(block, jnp.int32),
            pltpu.VMEM((1, lanes), jnp.float32),
            pltpu.VMEM((1, lanes), jnp.float32),
            pltpu.SMEM((1,), jnp.float32),
            pltpu.SMEM((1,), jnp.float32),
            pltpu.VMEM((rows // SUB, SUB, lanes), jnp.float32),
            pltpu.VMEM((rows // SUB, SUB, lanes), jnp.float32),
            pltpu.VMEM((T, E, ROWS, lanes), jnp.float32),
            pltpu.VMEM((T, E, lanes), jnp.float32),
            pltpu.SemaphoreType.DMA((6,)),
            pltpu.SemaphoreType.DMA((T * E - 1,)),
            pltpu.SemaphoreType.DMA((T * E - 1,)),
        ],
        compiler_params=pltpu.CompilerParams(collective_id=0, has_side_effects=True),
    )(rewards, dones, horizon.reshape(1, lanes), bootstrap.reshape(1, lanes), prior_mean, prior_var)
    return pl.pallas_call(
        functools.partial(finish, T, E),
        out_shape=(jax.ShapeDtypeStruct(block, jnp.float32),
                   jax.ShapeDtypeStruct(block, jnp.float32),
                   jax.ShapeDtypeStruct((2,), jnp.float32)),
        in_specs=[vmem] * 4,
        out_specs=(hbm, hbm, smem),
        scratch_shapes=[
            pltpu.VMEM(block, jnp.float32),
            pltpu.VMEM(block, jnp.float32),
            pltpu.SemaphoreType.DMA((2, PARTS)),
        ],
        compiler_params=pltpu.CompilerParams(vmem_limit_bytes=4 * 2**20),
    )(kept, returns, sums, prior)


def solution(mesh):
    T, E = mesh.shape["tm"], mesh.shape["env"]
    return jax.shard_map(
        functools.partial(local, T, E),
        mesh=mesh,
        in_specs=(P("tm", "env"), P("tm", "env"), P("env"), P("env"), P(), P()),
        out_specs=(P("tm", "env"), P("tm", "env"), P()),
        check_vma=False,
    )
```

```python
import functools

import jax
import jax.numpy as jnp
from jax import lax
from jax.experimental import pallas as pl
from jax.experimental.pallas import tpu as pltpu
from jax.sharding import PartitionSpec as P

SUB = 8
ROWS = 8
PARTS = 2


def compose_rows(summed, product, row):
    step = 1
    while step < SUB:
        inside = row < SUB - step
        later_sum = jnp.where(inside, pltpu.roll(summed, SUB - step, 0), 0.0)
        later_product = jnp.where(inside, pltpu.roll(product, SUB - step, 0), 1.0)
        summed = summed + product * later_sum
        product = product * later_product
        step *= 2
    return summed, product


def kernel(T, E, rewards_hbm, dones_hbm, horizon_hbm, bootstrap_hbm, mean_hbm, var_hbm,
           rewards, s_buf, p_buf, carry_ref, ebuf, prior_ref,
           dones, horizon_ref, bootstrap_ref, mean_ref, var_ref, tbuf, xbuf,
           load_sem, tsend, trecv):
    t = lax.axis_index("tm")
    e = lax.axis_index("env")
    barrier = pltpu.get_barrier_semaphore()
    offsets = [(i, j) for i in range(T) for j in range(E) if i or j]
    offsets.sort(key=lambda o: -min(o[0], T - o[0]))
    peers = [{"tm": lax.rem(t + i, T), "env": lax.rem(e + j, E)} for i, j in offsets]
    for peer in peers:
        pl.semaphore_signal(barrier, inc=1, device_id=peer, device_id_type=pl.DeviceIdType.MESH)
    pairs = [(horizon_hbm, horizon_ref), (mean_hbm, mean_ref), (var_hbm, var_ref),
             (bootstrap_hbm, bootstrap_ref), (rewards_hbm, rewards),
             (dones_hbm, dones)]
    loads = [pltpu.make_async_copy(source, target, load_sem.at[i])
             for i, (source, target) in enumerate(pairs)]
    for load in loads:
        load.start()
    rows, lanes = rewards.shape
    chunk = rows // SUB
    shape = (SUB, lanes)
    row = lax.broadcasted_iota(jnp.int32, shape, 0)
    for load in loads:
        load.wait()
    discount = jnp.broadcast_to(1.0 - 1.0 / horizon_ref[...], shape)
    center = jnp.full(shape, mean_ref[0], jnp.float32)
    s = jnp.zeros(shape, jnp.float32)
    p = jnp.ones(shape, jnp.float32)
    zero = jnp.zeros(shape, jnp.float32)
    s1, p1, s2, sp, p2 = zero, zero, zero, zero, zero
    for k in reversed(range(chunk)):
        r = rewards[pl.ds(k, SUB, stride=chunk), :]
        f = jnp.where(dones[pl.ds(k, SUB, stride=chunk), :] == 0, discount, 0.0)
        s = r + f * s
        p = f * p
        s_buf[k] = s
        p_buf[k] = p
        c = s - center
        s1 = s1 + c
        p1 = p1 + p
        s2 = s2 + c * c
        sp = sp + c * p
        p2 = p2 + p * p
    full_s, full_p = compose_rows(s, p, row)
    last = row == SUB - 1
    a = jnp.where(last, 0.0, pltpu.roll(full_s, SUB - 1, 0))
    b = jnp.where(last, 1.0, pltpu.roll(full_p, SUB - 1, 0))
    down = lambda value: jnp.sum(value, axis=0, keepdims=True)
    tbuf[t, e, 0:1] = full_s[0:1]
    tbuf[t, e, 1:2] = full_p[0:1]
    tbuf[t, e, 2:3] = down(s1 + p1 * a)
    tbuf[t, e, 3:4] = down(p1 * b)
    tbuf[t, e, 4:5] = down(s2 + a * (2.0 * sp + a * p2))
    tbuf[t, e, 5:6] = down(2.0 * b * (sp + a * p2))
    tbuf[t, e, 6:7] = down(b * b * p2)
    tbuf[t, e, 7:8] = bootstrap_ref[...]
    pl.semaphore_wait(barrier, T * E - 1)
    copies = [pltpu.make_async_remote_copy(
        tbuf.at[t, e], tbuf.at[t, e], tsend.at[i], trecv.at[i],
        device_id=peer, device_id_type=pl.DeviceIdType.MESH) for i, peer in enumerate(peers)]
    for copy in copies:
        copy.start()
    for copy in copies:
        copy.wait()
    x = tbuf[T - 1, :, 7]
    first = jnp.zeros((E, lanes), jnp.float32)
    second = jnp.zeros((E, lanes), jnp.float32)
    for j in reversed(range(T)):
        xbuf[j] = x
        first = first + tbuf[j, :, 2] + tbuf[j, :, 3] * x
        second = second + tbuf[j, :, 4] + x * (tbuf[j, :, 5] + x * tbuf[j, :, 6])
        x = tbuf[j, :, 0] + tbuf[j, :, 1] * x
    mine = xbuf[t, pl.ds(e, 1), :]
    ebuf[0] = first
    ebuf[1] = second
    prior_ref[0:1] = center[0:1]
    prior_ref[1:2] = jnp.full((1, lanes), var_ref[0], jnp.float32)
    carry_ref[...] = a + b * mine


def finish(T, E, rewards, s_buf, p_buf, carry_ref, ebuf, prior_ref, out_rewards, out_returns, out_stats,
           rewards_out, returns_out, stats, sems):
    rows, lanes = rewards.shape
    chunk = rows // SUB
    first = jnp.sum(jnp.sum(ebuf[0], axis=0, keepdims=True), axis=1, keepdims=True)
    second = jnp.sum(jnp.sum(ebuf[1], axis=0, keepdims=True), axis=1, keepdims=True)
    entries = float(rows * T * lanes * E)
    prior_count = entries
    merged = prior_count + entries
    mean0 = prior_ref[0:1, 0:1]
    var0 = prior_ref[1:2, 0:1]
    delta = first * (1.0 / entries)
    spread = second - first * delta
    new_mean = mean0 + delta * (entries / merged)
    variance = (var0 * (prior_count / merged) + spread * (1.0 / merged)
                + delta * delta * (prior_count / merged * (entries / merged)))
    inverse = jnp.broadcast_to(lax.rsqrt(variance + 1e-08), (SUB, lanes))
    copies = []

    def send(source, target, rank):
        copy = pltpu.make_async_copy(source, target, sems.at[rank])
        copy.start()
        copies.append(copy)

    y = carry_ref[...] * inverse
    for k in range(chunk):
        returns_out[pl.ds(k, SUB, stride=chunk), :] = s_buf[k] * inverse + p_buf[k] * y
    send(returns_out, out_returns, 0)
    part = rows // PARTS
    for i in range(PARTS):
        for k in range(i * part, (i + 1) * part, SUB):
            rewards_out[k:k + SUB] = rewards[k:k + SUB] * inverse
        where = pl.ds(i * part, part)
        send(rewards_out.at[where], out_rewards.at[where], 2 + i)
    stats[0] = new_mean[0, 0]
    stats[1] = variance[0, 0]
    send(stats, out_stats, 1)
    for copy in copies:
        copy.wait()


def local(T, E, rewards, dones, horizon, bootstrap, prior_mean, prior_var):
    rows, lanes = rewards.shape
    block = (rows, lanes)
    vmem = pl.BlockSpec(memory_space=pltpu.VMEM)
    hbm = pl.BlockSpec(memory_space=pltpu.HBM)
    kept, summed, product, carry, sums, prior = pl.pallas_call(
        functools.partial(kernel, T, E),
        out_shape=(pltpu.VMEM(block, jnp.float32),
                   pltpu.VMEM((rows // SUB, SUB, lanes), jnp.float32),
                   pltpu.VMEM((rows // SUB, SUB, lanes), jnp.float32),
                   pltpu.VMEM((SUB, lanes), jnp.float32),
                   pltpu.VMEM((2, E, lanes), jnp.float32), pltpu.VMEM((2, lanes), jnp.float32)),
        in_specs=[hbm] * 6,
        out_specs=(vmem,) * 6,
        scratch_shapes=[
            pltpu.VMEM(block, jnp.int32),
            pltpu.VMEM((1, lanes), jnp.float32),
            pltpu.VMEM((1, lanes), jnp.float32),
            pltpu.SMEM((1,), jnp.float32),
            pltpu.SMEM((1,), jnp.float32),
            pltpu.VMEM((T, E, ROWS, lanes), jnp.float32),
            pltpu.VMEM((T, E, lanes), jnp.float32),
            pltpu.SemaphoreType.DMA((6,)),
            pltpu.SemaphoreType.DMA((T * E - 1,)),
            pltpu.SemaphoreType.DMA((T * E - 1,)),
        ],
        compiler_params=pltpu.CompilerParams(collective_id=0, has_side_effects=True),
    )(rewards, dones, horizon.reshape(1, lanes), bootstrap.reshape(1, lanes), prior_mean, prior_var)
    return pl.pallas_call(
        functools.partial(finish, T, E),
        out_shape=(jax.ShapeDtypeStruct(block, jnp.float32),
                   jax.ShapeDtypeStruct(block, jnp.float32),
                   jax.ShapeDtypeStruct((2,), jnp.float32)),
        in_specs=[vmem] * 6,
        out_specs=(hbm, hbm, hbm),
        scratch_shapes=[
            pltpu.VMEM(block, jnp.float32),
            pltpu.VMEM(block, jnp.float32),
            pltpu.SMEM((2,), jnp.float32),
            pltpu.SemaphoreType.DMA((2 + PARTS,)),
        ],
        compiler_params=pltpu.CompilerParams(vmem_limit_bytes=4 * 2**20),
    )(kept, summed, product, carry, sums, prior)


def solution(mesh):
    T, E = mesh.shape["tm"], mesh.shape["env"]
    return jax.shard_map(
        functools.partial(local, T, E),
        mesh=mesh,
        in_specs=(P("tm", "env"), P("tm", "env"), P("env"), P("env"), P(), P()),
        out_specs=(P("tm", "env"), P("tm", "env"), P()),
        check_vma=False,
    )
```

```python
import functools

import jax
import jax.numpy as jnp
from jax import lax
from jax.experimental import pallas as pl
from jax.experimental.pallas import tpu as pltpu
from jax.sharding import PartitionSpec as P

SUB = 8
ROWS = 8
SENT = 7
PARTS = 2


def compose_rows(summed, product, row):
    step = 1
    while step < SUB:
        inside = row < SUB - step
        later_sum = jnp.where(inside, pltpu.roll(summed, SUB - step, 0), 0.0)
        later_product = jnp.where(inside, pltpu.roll(product, SUB - step, 0), 1.0)
        summed = summed + product * later_sum
        product = product * later_product
        step *= 2
    return summed, product


def kernel(T, E, rewards_hbm, dones_hbm, horizon_hbm, bootstrap_hbm, mean_hbm, var_hbm,
           rewards, s_buf, p_buf, carry_ref, ebuf, prior_ref,
           dones, horizon_ref, bootstrap_ref, mean_ref, var_ref, tbuf, xbuf,
           load_sem, tsend, trecv):
    t = lax.axis_index("tm")
    e = lax.axis_index("env")
    barrier = pltpu.get_barrier_semaphore()
    offsets = [(i, j) for i in range(T) for j in range(E) if i or j]
    offsets.sort(key=lambda o: -min(o[0], T - o[0]))
    peers = [{"tm": lax.rem(t + i, T), "env": lax.rem(e + j, E)} for i, j in offsets]
    for peer in peers:
        pl.semaphore_signal(barrier, inc=1, device_id=peer, device_id_type=pl.DeviceIdType.MESH)
    pairs = [(horizon_hbm, horizon_ref), (mean_hbm, mean_ref), (var_hbm, var_ref),
             (bootstrap_hbm, bootstrap_ref), (rewards_hbm, rewards),
             (dones_hbm, dones)]
    loads = [pltpu.make_async_copy(source, target, load_sem.at[i])
             for i, (source, target) in enumerate(pairs)]
    for load in loads:
        load.start()
    rows, lanes = rewards.shape
    chunk = rows // SUB
    shape = (SUB, lanes)
    row = lax.broadcasted_iota(jnp.int32, shape, 0)
    for load in loads:
        load.wait()
    discount = jnp.broadcast_to(1.0 - 1.0 / horizon_ref[...], shape)
    center = jnp.full(shape, mean_ref[0], jnp.float32)
    s = jnp.zeros(shape, jnp.float32)
    p = jnp.ones(shape, jnp.float32)
    zero = jnp.zeros(shape, jnp.float32)
    s1, p1, s2, sp, p2 = zero, zero, zero, zero, zero
    for k in reversed(range(chunk)):
        r = rewards[pl.ds(k, SUB, stride=chunk), :]
        f = jnp.where(dones[pl.ds(k, SUB, stride=chunk), :] == 0, discount, 0.0)
        s = r + f * s
        p = f * p
        s_buf[k] = s
        p_buf[k] = p
        c = s - center
        s1 = s1 + c
        p1 = p1 + p
        s2 = s2 + c * c
        sp = sp + c * p
        p2 = p2 + p * p
    full_s, full_p = compose_rows(s, p, row)
    last = row == SUB - 1
    a = jnp.where(last, 0.0, pltpu.roll(full_s, SUB - 1, 0))
    b = jnp.where(last, 1.0, pltpu.roll(full_p, SUB - 1, 0))
    down = lambda value: jnp.sum(value, axis=0, keepdims=True)
    known = jnp.where(t == T - 1, bootstrap_ref[...], jnp.zeros((1, lanes), jnp.float32))
    a = a + b * known
    rest = sp + a * p2
    tbuf[t, e, 0:1] = full_s[0:1] + full_p[0:1] * known
    tbuf[t, e, 1:2] = full_p[0:1]
    tbuf[t, e, 2:3] = down(s1 + p1 * a)
    tbuf[t, e, 3:4] = down(p1 * b)
    tbuf[t, e, 4:5] = down(s2 + a * (sp + rest))
    tbuf[t, e, 5:6] = down(2.0 * b * rest)
    tbuf[t, e, 6:7] = down(b * b * p2)
    pl.semaphore_wait(barrier, T * E - 1)
    copies = [pltpu.make_async_remote_copy(
        tbuf.at[t, e, 0:SENT], tbuf.at[t, e, 0:SENT], tsend.at[i], trecv.at[i],
        device_id=peer, device_id_type=pl.DeviceIdType.MESH) for i, peer in enumerate(peers)]
    for copy in copies:
        copy.start()
    for copy in copies:
        copy.wait()
    x = jnp.zeros((E, lanes), jnp.float32)
    first = jnp.zeros((E, lanes), jnp.float32)
    second = jnp.zeros((E, lanes), jnp.float32)
    for j in reversed(range(T)):
        xbuf[j] = x
        first = first + tbuf[j, :, 2] + tbuf[j, :, 3] * x
        second = second + tbuf[j, :, 4] + x * (tbuf[j, :, 5] + x * tbuf[j, :, 6])
        x = tbuf[j, :, 0] + tbuf[j, :, 1] * x
    mine = xbuf[t, pl.ds(e, 1), :]
    ebuf[0] = first
    ebuf[1] = second
    prior_ref[0:1] = center[0:1]
    prior_ref[1:2] = jnp.full((1, lanes), var_ref[0], jnp.float32)
    carry_ref[...] = a + b * mine


def finish(T, E, rewards, s_buf, p_buf, carry_ref, ebuf, prior_ref, out_rewards, out_returns, out_stats,
           rewards_out, returns_out, stats, sems):
    rows, lanes = rewards.shape
    chunk = rows // SUB
    first = jnp.sum(jnp.sum(ebuf[0], axis=0, keepdims=True), axis=1, keepdims=True)
    second = jnp.sum(jnp.sum(ebuf[1], axis=0, keepdims=True), axis=1, keepdims=True)
    entries = float(rows * T * lanes * E)
    prior_count = entries
    merged = prior_count + entries
    mean0 = prior_ref[0:1, 0:1]
    var0 = prior_ref[1:2, 0:1]
    delta = first * (1.0 / entries)
    spread = second - first * delta
    new_mean = mean0 + delta * (entries / merged)
    variance = (var0 * (prior_count / merged) + spread * (1.0 / merged)
                + delta * delta * (prior_count / merged * (entries / merged)))
    inverse = jnp.broadcast_to(lax.rsqrt(variance + 1e-08), (SUB, lanes))
    copies = []

    def send(source, target, rank):
        copy = pltpu.make_async_copy(source, target, sems.at[rank])
        copy.start()
        copies.append(copy)

    y = carry_ref[...] * inverse
    for k in range(chunk):
        returns_out[pl.ds(k, SUB, stride=chunk), :] = s_buf[k] * inverse + p_buf[k] * y
    send(returns_out, out_returns, 0)
    part = rows // PARTS
    for i in range(PARTS):
        for k in range(i * part, (i + 1) * part, SUB):
            rewards_out[k:k + SUB] = rewards[k:k + SUB] * inverse
        where = pl.ds(i * part, part)
        send(rewards_out.at[where], out_rewards.at[where], 2 + i)
    stats[0] = new_mean[0, 0]
    stats[1] = variance[0, 0]
    send(stats, out_stats, 1)
    for copy in copies:
        copy.wait()


def local(T, E, rewards, dones, horizon, bootstrap, prior_mean, prior_var):
    rows, lanes = rewards.shape
    block = (rows, lanes)
    vmem = pl.BlockSpec(memory_space=pltpu.VMEM)
    hbm = pl.BlockSpec(memory_space=pltpu.HBM)
    kept, summed, product, carry, sums, prior = pl.pallas_call(
        functools.partial(kernel, T, E),
        out_shape=(pltpu.VMEM(block, jnp.float32),
                   pltpu.VMEM((rows // SUB, SUB, lanes), jnp.float32),
                   pltpu.VMEM((rows // SUB, SUB, lanes), jnp.float32),
                   pltpu.VMEM((SUB, lanes), jnp.float32),
                   pltpu.VMEM((2, E, lanes), jnp.float32), pltpu.VMEM((2, lanes), jnp.float32)),
        in_specs=[hbm] * 6,
        out_specs=(vmem,) * 6,
        scratch_shapes=[
            pltpu.VMEM(block, jnp.int32),
            pltpu.VMEM((1, lanes), jnp.float32),
            pltpu.VMEM((1, lanes), jnp.float32),
            pltpu.SMEM((1,), jnp.float32),
            pltpu.SMEM((1,), jnp.float32),
            pltpu.VMEM((T, E, ROWS, lanes), jnp.float32),
            pltpu.VMEM((T, E, lanes), jnp.float32),
            pltpu.SemaphoreType.DMA((6,)),
            pltpu.SemaphoreType.DMA((T * E - 1,)),
            pltpu.SemaphoreType.DMA((T * E - 1,)),
        ],
        compiler_params=pltpu.CompilerParams(collective_id=0, has_side_effects=True),
    )(rewards, dones, horizon.reshape(1, lanes), bootstrap.reshape(1, lanes), prior_mean, prior_var)
    return pl.pallas_call(
        functools.partial(finish, T, E),
        out_shape=(jax.ShapeDtypeStruct(block, jnp.float32),
                   jax.ShapeDtypeStruct(block, jnp.float32),
                   jax.ShapeDtypeStruct((2,), jnp.float32)),
        in_specs=[vmem] * 6,
        out_specs=(hbm, hbm, hbm),
        scratch_shapes=[
            pltpu.VMEM(block, jnp.float32),
            pltpu.VMEM(block, jnp.float32),
            pltpu.SMEM((2,), jnp.float32),
            pltpu.SemaphoreType.DMA((2 + PARTS,)),
        ],
        compiler_params=pltpu.CompilerParams(vmem_limit_bytes=4 * 2**20),
    )(kept, summed, product, carry, sums, prior)


def solution(mesh):
    T, E = mesh.shape["tm"], mesh.shape["env"]
    return jax.shard_map(
        functools.partial(local, T, E),
        mesh=mesh,
        in_specs=(P("tm", "env"), P("tm", "env"), P("env"), P("env"), P(), P()),
        out_specs=(P("tm", "env"), P("tm", "env"), P()),
        check_vma=False,
    )
```
